32 devices in a mesh: dp: 4 (over z), head: 8 (over y, x, core).
Axes of the slice: x: 2, y: 2, z: 4, core: 2. Of those that a mesh axis runs over, the one named last changes fastest.
Arguments:
- projected: bfloat16 [12288, 24576], P(('dp', 'head')), may hold values from -64 to 64, as said below
- weight_exp: int32 [12288], P(('dp', 'head')), may hold values from 0 to 3
- damp_exp: int32 [128], replicated, may hold values from 0 to 2
Outputs:
- whitening: float32 [128, 192, 192], P('head')
The draws below stay inside these ranges and needn't reach their ends.
Inputs may be any that keep to these rules, and one draw needn't show every extreme that they name: `projected`: real values.
All inputs are finite; a program needn't handle non-finite values.
Results may differ from the reference program's by a relative error of at most 0.0003.
Values may be sent and summed in bfloat16 or wider, within the bound.
A program may use at most 192 MiB of HBM per device.

```python
import math
import jax
import jax.numpy as jnp
from jax import lax

HEADS = 64
HD = 192
TOKENS = 12288
MATS = 128


def draw_projected(key, part):
    first, second = jax.random.split(jax.random.fold_in(key, 11))
    base = jax.random.normal(first, (TOKENS, 2 * HEADS, HD), jnp.float32)
    scales = jnp.exp(jax.random.uniform(second, (2 * HEADS, HD), jnp.float32, 0.0, math.log(8.0)))
    mixed = base + 0.6 * jnp.roll(base, 1, axis=2) - 0.4 * jnp.roll(base, 5, axis=2)
    return jnp.clip((mixed * scales).reshape(TOKENS, 2 * HEADS * HD) / 4.0, -64.0, 64.0).astype(jnp.bfloat16)


def place_ends(entries, own_key, smallest, largest):
    longest = entries.shape.index(max(entries.shape))
    spots = []
    for shift in (0, 1):
        where = [jax.random.randint(jax.random.fold_in(own_key, axis), (), 0, length) for axis, length in enumerate(entries.shape)]
        where[longest] = (where[longest] + shift) % entries.shape[longest]
        spots.append(tuple(where))
    return entries.at[spots[0]].set(smallest).at[spots[1]].set(largest)


def setup_inputs(seed: int = 0) -> dict:
    seeds = jax.random.split(jax.random.key(seed), 4)
    return {
        "projected": draw_projected(jax.random.fold_in(seeds[3], 71), 0),
        "weight_exp": place_ends(jax.random.randint(seeds[1], (TOKENS,), 0, 4), jax.random.fold_in(seeds[1], 1), 0, 3).astype(jnp.int32),
        "damp_exp": place_ends(jax.random.randint(seeds[2], (MATS,), 0, 3), jax.random.fold_in(seeds[2], 1), 0, 2).astype(jnp.int32),
    }


def reference(projected, weight_exp, damp_exp):
    mats = projected.shape[1] // HD
    weights = jnp.exp2(weight_exp.astype(jnp.float32)).astype(jnp.bfloat16)
    scaled = projected * weights[:, None]
    eye = jnp.eye(HD, dtype=jnp.float32)

    def single(index):
        start = (index * HD).astype(jnp.int32)
        left = lax.dynamic_slice_in_dim(projected, start, HD, 1)
        right = lax.dynamic_slice_in_dim(scaled, start, HD, 1)
        gram = jnp.dot(left.T.astype(jnp.float32), right.astype(jnp.float32), preferred_element_type=jnp.float32) / TOKENS
        gram = 0.5 * (gram + gram.T)
        level = jnp.trace(gram) / HD + 1e-06
        damping = jnp.exp2(-damp_exp[index].astype(jnp.float32)) * level
        lower = jnp.linalg.cholesky(gram + damping * eye)
        return jax.scipy.linalg.solve_triangular(lower, eye, lower=True)
    return lax.map(single, jnp.arange(mats, dtype=jnp.int32))
```

```python
import functools

import jax
import jax.numpy as jnp
from jax import lax
from jax.experimental import pallas as pl
from jax.experimental.pallas import tpu as pltpu
from jax.sharding import PartitionSpec as P

HD = 192
BLK = HD // 3
HIGH = lax.Precision.HIGHEST
LEVELS = 32767.0
TINY = 1e-30


def store_pair(rows, wide, out, at):
    weighted = rows * wide
    contract = (((0,), (0,)), ((), ()))
    width = 4 * BLK
    first = lax.dot_general(rows[:, :width], weighted[:, :width], contract, preferred_element_type=jnp.float32)
    second = lax.dot_general(rows[:, -width:], weighted[:, -width:], contract, preferred_element_type=jnp.float32)
    two = 2 * BLK
    lanes = lax.broadcasted_iota(jnp.int32, (BLK, two), 1)
    corner = pltpu.roll(first[two : two + BLK, two:], BLK, 1)
    out[at, :BLK, :] = jnp.where(lanes < BLK, first[:BLK, :two], corner)
    out[at, BLK:, :] = first[BLK:HD, :two]
    out[at + 1, :two, :] = second[BLK : BLK + two, two:]
    corner = pltpu.roll(second[BLK:two, :two], BLK, 1)
    out[at + 1, two:, :] = jnp.where(lanes < BLK, corner, second[HD:, two:])


def dot(a, b):
    return lax.dot_general(a, b, (((1,), (0,)), ((), ())), precision=HIGH, preferred_element_type=jnp.float32)


def dot_t(a, b):
    return lax.dot_general(a, b, (((1,), (1,)), ((), ())), precision=HIGH, preferred_element_type=jnp.float32)


def inverse_factors(blocks):
    lane = lax.broadcasted_iota(jnp.int32, (8, BLK), 1)
    sub = lax.broadcasted_iota(jnp.int32, (8, BLK), 0)
    sub1 = lax.broadcasted_iota(jnp.int32, (8, 1), 0)
    groups = BLK // 8
    held = [[block[8 * g : 8 * g + 8] for g in range(groups)] for block in blocks]
    for k in range(BLK):
        own, spot = divmod(k, 8)
        is_k = lane == k
        for parts in held:
            row = parts[own][spot : spot + 1, :]
            scale = 1.0 / row[:, k : k + 1]
            row = jnp.where(is_k[:1], 1.0, row) * scale
            for g in range(own, groups):
                part = parts[g]
                column = part[:, k : k + 1]
                if g == own:
                    if spot == 7:
                        continue
                    column = jnp.where(sub1 > spot, column, 0.0)
                    kept = jnp.where(is_k & (sub > spot), 0.0, part)
                else:
                    kept = jnp.where(is_k, 0.0, part)
                parts[g] = kept - column * row
    out = []
    for parts in held:
        rows = []
        for g in range(groups):
            ids = sub + 8 * g
            pivot = jnp.sum(jnp.where(lane == ids, parts[g], 0.0), axis=1, keepdims=True)
            unit = jnp.where(lane < ids, parts[g], jnp.where(lane == ids, 1.0, 0.0))
            rows.append(unit * (1.0 / jnp.sqrt(pivot)))
        out.append(jnp.concatenate(rows, axis=0))
    return out


def unpack_even(got):
    two = 2 * BLK
    return got[:BLK, :BLK], got[BLK:two, BLK:], got[:BLK, BLK:], got[BLK:, :BLK], got[two:, BLK:]


def unpack_odd(got):
    two = 2 * BLK
    return got[two:, :BLK], got[BLK:two, :BLK], got[two:, BLK:], got[:BLK, :].T, got[BLK:two, BLK:].T


def encode(value, scale):
    return jnp.round(value * scale).astype(jnp.int32).astype(jnp.int16)


def decode(code):
    return code.astype(jnp.int32).astype(jnp.float32)


def whiten_kernel(total, count, damp_ref, packed_ref, out_ref, step_ref):
    two = 2 * BLK
    diag = lax.broadcasted_iota(jnp.int32, (BLK, BLK), 0) == lax.broadcasted_iota(jnp.int32, (BLK, BLK), 1)
    a11, a22, a33, low, a32 = [], [], [], [], []
    for m in range(count):
        got = packed_ref[m] / total
        even = unpack_even(got)
        odd = unpack_odd(got)
        if count % 2 == 0:
            d1, d2, d3, left, corner = odd if m % 2 else even
        else:
            turn = (lax.axis_index("head") * lax.axis_size("dp") + lax.axis_index("dp")) * count + m
            d1, d2, d3, left, corner = (jnp.where(turn % 2 == 0, a, b) for a, b in zip(even, odd))
        trace = jnp.sum(jnp.where(diag, d1 + d2 + d3, 0.0), axis=(0, 1), keepdims=True)
        level = trace / HD + 1e-06
        shift = jnp.where(diag, damp_ref[m] * level, 0.0)
        a11.append(d1 + shift)
        a22.append(d2 + shift)
        a33.append(d3 + shift)
        low.append(left)
        a32.append(corner)
    each = range(count)
    w11 = inverse_factors(a11)
    l1 = [dot_t(low[m], w11[m]) for m in each]
    square = [dot_t(l1[m], l1[m]) for m in each]
    w22 = inverse_factors([a22[m] - square[m][:BLK, :BLK] for m in each])
    l32 = [dot_t(a32[m] - square[m][BLK:, :BLK], w22[m]) for m in each]
    w33 = inverse_factors([a33[m] - square[m][BLK:, BLK:] - dot_t(l32[m], l32[m]) for m in each])
    for m in each:
        below = dot(l1[m], w11[m])
        w21 = -dot(w22[m], below[:BLK])
        w32 = -dot(w33[m], dot(l32[m], w22[m]))
        w31 = -dot(w33[m], below[BLK:] + dot(l32[m], w21))
        bands = ((w11[m], w33[m]), (w21, w22[m]), (w31, w32))
        bands = [jnp.concatenate(band, axis=1) for band in bands]
        top = functools.reduce(jnp.maximum, [jnp.max(jnp.abs(band), axis=0, keepdims=True) for band in bands])
        top = jnp.maximum(top, TINY)
        step_ref[m] = top / LEVELS
        for n, band in enumerate(bands):
            out_ref[m, n * BLK : (n + 1) * BLK] = encode(band, LEVELS / top)


def whiten(packed, damp, total):
    count = packed.shape[0]
    return pl.pallas_call(
        functools.partial(whiten_kernel, total, count),
        in_specs=[pl.BlockSpec(memory_space=pltpu.SMEM), pl.BlockSpec(memory_space=pltpu.VMEM)],
        out_specs=[pl.BlockSpec(memory_space=pltpu.VMEM)] * 2,
        out_shape=[
            jax.ShapeDtypeStruct(packed.shape, jnp.int16),
            jax.ShapeDtypeStruct((count, 1, packed.shape[2]), jnp.float32),
        ],
    )(damp, packed)


def flip(index, step):
    return index + step * (1 - 2 * ((index // step) % 2))


def remote(src, dst, sems, slot, device):
    return pltpu.make_async_remote_copy(
        src_ref=src,
        dst_ref=dst,
        send_sem=sems.at[0, slot],
        recv_sem=sems.at[1, slot],
        device_id=device,
        device_id_type=pl.DeviceIdType.MESH,
    )


def greet(heads, dps):
    barrier = pltpu.get_barrier_semaphore()
    for peer in heads:
        pl.semaphore_signal(barrier, inc=1, device_id={"head": peer}, device_id_type=pl.DeviceIdType.MESH)
    for peer in dps:
        pl.semaphore_signal(barrier, inc=1, device_id={"dp": peer}, device_id_type=pl.DeviceIdType.MESH)
    pl.semaphore_wait(barrier, len(heads) + len(dps))


def part_rows():
    last = HD // 4
    first = (HD - last) // 2
    return (0, first), (first, first), (2 * first, last)


def scatter_kernel(n_head, n_dp, share, rows_ref, weights_ref, out_ref, acc, sent, own_grams, wide, columns, got_a, got_b, got_c, got_z, got_y, sem_in, sem_0, sem_a, sem_b, sem_c, sem_z, sem_y):
    head = lax.axis_index("head")
    dp = lax.axis_index("dp")
    chunks = n_head // 2
    bits = chunks.bit_length() - 1
    mine = head // 2
    core = head % 2
    per_head = share * n_dp
    span = per_head * HD
    peers = [lax.rem(dp + o, n_dp) for o in range(1, n_dp)]
    part_a, part_b, part_c = part_rows()
    up = list(range(bits))
    down = up[::-1]
    rows_c = pl.ds(part_c[0], part_c[1])

    def chunk_of(e):
        chunk = mine
        for j in range(bits):
            if (e >> j) & 1:
                chunk = chunk + (1 - 2 * ((mine // (1 << j)) % 2)) * (1 << j)
        return chunk

    order = list(range(chunks))[::-1]
    visits = []
    for e in order:
        visits += [2 * chunk_of(e) + 1 - core, 2 * chunk_of(e) + core]

    def fetch(v):
        start = pl.multiple_of(visits[v] * span, 2 * BLK)
        return pltpu.make_async_copy(rows_ref.at[:, pl.ds(start, span)], columns.at[v % 2], sem_in.at[v % 2])

    fetch(0).start()
    wide[...] = jnp.broadcast_to(weights_ref[...], wide.shape)
    greet([flip(head, 1 << j) for j in range(bits + 1)], peers)

    def multiply(v, out):
        if v + 1 < len(visits):
            fetch(v + 1).start()
        fetch(v).wait()

        def pair(i, carry):
            start = pl.multiple_of(i * 2 * HD, 2 * BLK)
            store_pair(columns[v % 2, :, pl.ds(start, 2 * HD)], wide[...], out, 2 * i)
            return carry

        lax.fori_loop(0, per_head // 2, pair, 0, unroll=2)

    def squeeze(e, j):
        return (e >> (j + 1) << j) | (e & ((1 << j) - 1))

    early = {"a": [], "b": []}
    flight_z = []
    for n, e in enumerate(order):
        c = chunk_of(e)
        multiply(2 * n, sent.at[n])
        copy = remote(sent.at[n], acc.at[c], sem_0, n, {"head": flip(head, 1)})
        copy.start()
        multiply(2 * n + 1, own_grams)
        copy.wait()

        def add(m, carry, c=c):
            acc[c, m] += own_grams[m]
            return carry

        lax.fori_loop(0, per_head, add, 0)
        for name, (start, size), got, sems, j in (("a", part_a, got_a, sem_a, up[0]), ("b", part_b, got_b, sem_b, down[0])):
            if (e >> j) & 1:
                slot = squeeze(e, j)
                out = remote(
                    acc.at[c, pl.ds(0, per_head), pl.ds(start, size)], got.at[slot], sems, slot, {"head": flip(head, 2 << j)}
                )
                out.start()
                early[name].append((out, chunk_of(e ^ (1 << j)), slot))
        for o, peer in enumerate(peers):
            out = remote(
                acc.at[c, pl.ds(peer * share, share), rows_c], got_z.at[o, e], sem_z, o * chunks + e, {"dp": peer}
            )
            out.start()
            flight_z.append(out)

    def begin(part, got, sems, order, step, first, count):
        j = order[step]
        bit = (mine // (1 << j)) % 2
        fixed = 0
        for done in order[:step]:
            fixed = fixed + (mine // (1 << done)) % 2 * (1 << done)
        free = [b for b in range(bits) if b not in order[: step + 1]]
        flight = []
        start, size = part
        offset = sum(chunks >> (s + 1) for s in range(step))
        for e in range(1 << len(free)):
            base = fixed + sum(((e >> i) & 1) << b for i, b in enumerate(free))
            slot = offset + e
            copy = remote(
                acc.at[base + (1 - bit) * (1 << j), pl.ds(first, count), pl.ds(start, size)],
                got.at[slot],
                sems,
                slot,
                {"head": flip(head, 2 << j)},
            )
            copy.start()
            flight.append((copy, base + bit * (1 << j), slot))
        return flight, part, got, first, count

    def finish(state):
        flight, (start, size), got, first, count = state
        for copy, keep, slot in flight:
            copy.wait()

            def add(m, carry, keep=keep, slot=slot):
                acc[keep, first + m, start : start + size] += got[slot, m]
                return carry

            lax.fori_loop(0, count, add, 0)

    own = dp * share
    for step in range(bits):
        if step:
            state_a = begin(part_a, got_a, sem_a, up, step, 0, per_head)
            state_b = begin(part_b, got_b, sem_b, down, step, 0, per_head)
        else:
            state_a = early["a"], part_a, got_a, 0, per_head
            state_b = early["b"], part_b, got_b, 0, per_head
        finish(state_a)
        finish(state_b)
    rows_ab = pl.ds(0, part_c[0])
    flight_y = []
    for o, peer in enumerate(peers):
        copy = remote(acc.at[mine, pl.ds(peer * share, share), rows_ab], got_y.at[o], sem_y, o, {"dp": peer})
        copy.start()
        flight_y.append(copy)
    for copy in flight_z:
        copy.wait()
    for e in range(chunks):

        def add_z(m, carry, c=chunk_of(e), e=e):
            value = acc[c, own + m, part_c[0] :]
            for o in range(len(peers)):
                value += got_z[o, e, m]
            acc[c, own + m, part_c[0] :] = value
            return carry

        lax.fori_loop(0, share, add_z, 0)
    for step in range(bits):
        finish(begin(part_c, got_c, sem_c, up, step, own, share))
    for copy in flight_y:
        copy.wait()

    def add_y(m, carry):
        value = acc[mine, own + m, : part_c[0]]
        for o in range(len(peers)):
            value += got_y[o, m]
        out_ref[m, : part_c[0]] = value
        out_ref[m, part_c[0] :] = acc[mine, own + m, part_c[0] :]
        return carry

    lax.fori_loop(0, share, add_y, 0)


def gram_sums(projected, weights, n_head, n_dp):
    tokens, width = projected.shape
    mats, rows, lanes = width // HD, HD, 2 * BLK
    per_head = mats // n_head
    share = per_head // n_dp
    chunks = n_head // 2
    (_, rows_a), (_, rows_b), (_, rows_c) = part_rows()
    f32 = jnp.float32
    return pl.pallas_call(
        functools.partial(scatter_kernel, n_head, n_dp, share),
        in_specs=[pl.BlockSpec(memory_space=pl.ANY), pl.BlockSpec(memory_space=pltpu.VMEM)],
        out_specs=pl.BlockSpec(memory_space=pltpu.VMEM),
        out_shape=jax.ShapeDtypeStruct((share, rows, lanes), f32),
        scratch_shapes=[
            pltpu.VMEM((chunks, per_head, rows, lanes), f32),
            pltpu.VMEM((chunks, per_head, rows, lanes), f32),
            pltpu.VMEM((per_head, rows, lanes), f32),
            pltpu.VMEM((tokens, 2 * HD), projected.dtype),
            pltpu.VMEM((2, tokens, per_head * HD), projected.dtype),
            pltpu.VMEM((chunks - 1, per_head, rows_a, lanes), f32),
            pltpu.VMEM((chunks - 1, per_head, rows_b, lanes), f32),
            pltpu.VMEM((chunks - 1, share, rows_c, lanes), f32),
            pltpu.VMEM((n_dp - 1, chunks, share, rows_c, lanes), f32),
            pltpu.VMEM((n_dp - 1, share, rows - rows_c, lanes), f32),
            pltpu.SemaphoreType.DMA((2,)),
            pltpu.SemaphoreType.DMA((2, chunks)),
            pltpu.SemaphoreType.DMA((2, chunks - 1)),
            pltpu.SemaphoreType.DMA((2, chunks - 1)),
            pltpu.SemaphoreType.DMA((2, chunks - 1)),
            pltpu.SemaphoreType.DMA((2, (n_dp - 1) * chunks)),
            pltpu.SemaphoreType.DMA((2, n_dp - 1)),
        ],
        compiler_params=pltpu.CompilerParams(collective_id=0, has_side_effects=True, vmem_limit_bytes=60 << 20),
    )(projected, weights)


def gather_kernel(n_dp, share, code_ref, step_ref, codes, steps, sems, step_sems, own_sems):
    dp = lax.axis_index("dp")
    peers = [lax.rem(dp + o, n_dp) for o in range(1, n_dp)]
    mine = pl.ds(dp * share, share)
    own = [
        pltpu.make_async_copy(code_ref, codes.at[mine], own_sems.at[0]),
        pltpu.make_async_copy(step_ref, steps.at[mine], own_sems.at[1]),
    ]
    for copy in own:
        copy.start()
    greet([], peers)
    flight = []
    for o, peer in enumerate(peers):
        flight.append(remote(code_ref, codes.at[mine], sems, o, {"dp": peer}))
        flight.append(remote(step_ref, steps.at[mine], step_sems, o, {"dp": peer}))
    for copy in flight:
        copy.start()
    for copy in own + flight:
        copy.wait()


def gather(code, step, n_dp):
    share = code.shape[0]
    return pl.pallas_call(
        functools.partial(gather_kernel, n_dp, share),
        in_specs=[pl.BlockSpec(memory_space=pltpu.VMEM)] * 2,
        out_specs=[pl.BlockSpec(memory_space=pltpu.VMEM)] * 2,
        out_shape=[
            jax.ShapeDtypeStruct((n_dp * share, *code.shape[1:]), code.dtype),
            jax.ShapeDtypeStruct((n_dp * share, *step.shape[1:]), step.dtype),
        ],
        scratch_shapes=[
            pltpu.SemaphoreType.DMA((2, n_dp - 1)),
            pltpu.SemaphoreType.DMA((2, n_dp - 1)),
            pltpu.SemaphoreType.DMA((2,)),
        ],
        compiler_params=pltpu.CompilerParams(collective_id=1, has_side_effects=True),
    )(code, step)


def unpack_kernel(code_ref, step_ref, out_ref):
    two = 2 * BLK
    left = lax.broadcasted_iota(jnp.int32, (BLK, two), 1) < BLK
    for m in range(out_ref.shape[0]):
        step = step_ref[m]
        top = decode(code_ref[m, :BLK]) * step
        out_ref[m, :BLK, :two] = jnp.where(left, top, 0.0)
        out_ref[m, BLK:, :two] = decode(code_ref[m, BLK:]) * step
        out_ref[m, :two, two:] = jnp.zeros((two, BLK), jnp.float32)
        out_ref[m, two:, two:] = top[:, BLK:]


def unpack(codes, steps):
    mats, rows, lanes = codes.shape
    group = 2
    return pl.pallas_call(
        unpack_kernel,
        grid=(mats // group,),
        in_specs=[
            pl.BlockSpec((group, rows, lanes), lambda i: (i, 0, 0)),
            pl.BlockSpec((group, 1, lanes), lambda i: (i, 0, 0)),
        ],
        out_specs=pl.BlockSpec((group, HD, HD), lambda i: (i, 0, 0)),
        out_shape=jax.ShapeDtypeStruct((mats, HD, HD), jnp.float32),
    )(codes, steps)


def on_device(projected, weight_exp, damp_exp):
    n_head = lax.axis_size("head")
    n_dp = lax.axis_size("dp")
    mats = projected.shape[1] // HD
    share = mats // (n_head * n_dp)
    total = projected.shape[0] * n_head * n_dp
    weights = jnp.exp2(weight_exp.astype(jnp.float32)).astype(jnp.bfloat16)
    owned = gram_sums(projected, weights[:, None], n_head, n_dp)
    first = (lax.axis_index("head") * n_dp + lax.axis_index("dp")) * share
    damp = jnp.exp2(-lax.dynamic_slice_in_dim(damp_exp, first, share, 0).astype(jnp.float32))
    code, step = whiten(owned, damp, float(total))
    codes, steps = gather(code, step, n_dp)
    return unpack(codes, steps)


def solution(mesh):
    return jax.shard_map(
        on_device,
        mesh=mesh,
        in_specs=(P(("dp", "head"), None), P(("dp", "head")), P()),
        out_specs=P("head", None, None),
        check_vma=False,
    )
```

```python
import functools
import math

import jax
import jax.numpy as jnp
from jax import lax
from jax.experimental import pallas as pl
from jax.experimental.pallas import tpu as pltpu
from jax.sharding import PartitionSpec as P

HD = 192
BLK = HD // 3
HIGH = lax.Precision.HIGHEST
LEVELS = 32767.0
TINY = 1e-30
DEPTH = 4
LAG = 3


def store_pair(rows, wide, out, at):
    weighted = rows * wide
    contract = (((0,), (0,)), ((), ()))
    width = 4 * BLK
    first = lax.dot_general(rows[:, :width], weighted[:, :width], contract, preferred_element_type=jnp.float32)
    second = lax.dot_general(rows[:, -width:], weighted[:, -width:], contract, preferred_element_type=jnp.float32)
    two = 2 * BLK
    lanes = lax.broadcasted_iota(jnp.int32, (BLK, two), 1)
    corner = pltpu.roll(first[two : two + BLK, two:], BLK, 1)
    out[at, :BLK, :] = jnp.where(lanes < BLK, first[:BLK, :two], corner)
    out[at, BLK:, :] = first[BLK:HD, :two]
    out[at + 1, :two, :] = second[BLK : BLK + two, two:]
    corner = pltpu.roll(second[BLK:two, :two], BLK, 1)
    out[at + 1, two:, :] = jnp.where(lanes < BLK, corner, second[HD:, two:])


def dot(a, b):
    return lax.dot_general(a, b, (((1,), (0,)), ((), ())), precision=HIGH, preferred_element_type=jnp.float32)


def dot_t(a, b):
    return lax.dot_general(a, b, (((1,), (1,)), ((), ())), precision=HIGH, preferred_element_type=jnp.float32)


def inverse_factors(blocks):
    lane = lax.broadcasted_iota(jnp.int32, (8, BLK), 1)
    sub = lax.broadcasted_iota(jnp.int32, (8, BLK), 0)
    sub1 = lax.broadcasted_iota(jnp.int32, (8, 1), 0)
    groups = BLK // 8
    held = [[block[8 * g : 8 * g + 8] for g in range(groups)] for block in blocks]
    for k in range(BLK):
        own, spot = divmod(k, 8)
        is_k = lane == k
        for parts in held:
            row = parts[own][spot : spot + 1, :]
            scale = 1.0 / row[:, k : k + 1]
            row = jnp.where(is_k[:1], 1.0, row) * scale
            for g in range(own, groups):
                part = parts[g]
                column = part[:, k : k + 1]
                if g == own:
                    if spot == 7:
                        continue
                    column = jnp.where(sub1 > spot, column, 0.0)
                    kept = jnp.where(is_k & (sub > spot), 0.0, part)
                else:
                    kept = jnp.where(is_k, 0.0, part)
                parts[g] = kept - column * row
    out = []
    for parts in held:
        rows = []
        for g in range(groups):
            ids = sub + 8 * g
            pivot = jnp.sum(jnp.where(lane == ids, parts[g], 0.0), axis=1, keepdims=True)
            unit = jnp.where(lane < ids, parts[g], jnp.where(lane == ids, 1.0, 0.0))
            rows.append(unit * (1.0 / jnp.sqrt(pivot)))
        out.append(jnp.concatenate(rows, axis=0))
    return out


def unpack_even(got):
    two = 2 * BLK
    return got[:BLK, :BLK], got[BLK:two, BLK:], got[:BLK, BLK:], got[BLK:, :BLK], got[two:, BLK:]


def unpack_odd(got):
    two = 2 * BLK
    return got[two:, :BLK], got[BLK:two, :BLK], got[two:, BLK:], got[:BLK, :].T, got[BLK:two, BLK:].T


def encode(value, scale):
    return jnp.round(value * scale).astype(jnp.int32).astype(jnp.int16)


def decode(code):
    return code.astype(jnp.int32).astype(jnp.float32)


def whiten_kernel(total, count, damp_ref, packed_ref, out_ref, step_ref):
    two = 2 * BLK
    diag = lax.broadcasted_iota(jnp.int32, (BLK, BLK), 0) == lax.broadcasted_iota(jnp.int32, (BLK, BLK), 1)
    a11, a22, a33, low, a32 = [], [], [], [], []
    for m in range(count):
        got = packed_ref[m] / total
        even = unpack_even(got)
        odd = unpack_odd(got)
        if count % 2 == 0:
            d1, d2, d3, left, corner = odd if m % 2 else even
        else:
            turn = (lax.axis_index("head") * lax.axis_size("dp") + lax.axis_index("dp")) * count + m
            d1, d2, d3, left, corner = (jnp.where(turn % 2 == 0, a, b) for a, b in zip(even, odd))
        trace = jnp.sum(jnp.where(diag, d1 + d2 + d3, 0.0), axis=(0, 1), keepdims=True)
        level = trace / HD + 1e-06
        shift = jnp.where(diag, damp_ref[m] * level, 0.0)
        a11.append(d1 + shift)
        a22.append(d2 + shift)
        a33.append(d3 + shift)
        low.append(left)
        a32.append(corner)
    each = range(count)
    w11 = inverse_factors(a11)
    l1 = [dot_t(low[m], w11[m]) for m in each]
    square = [dot_t(l1[m], l1[m]) for m in each]
    w22 = inverse_factors([a22[m] - square[m][:BLK, :BLK] for m in each])
    l32 = [dot_t(a32[m] - square[m][BLK:, :BLK], w22[m]) for m in each]
    w33 = inverse_factors([a33[m] - square[m][BLK:, BLK:] - dot_t(l32[m], l32[m]) for m in each])
    for m in each:
        below = dot(l1[m], w11[m])
        w21 = -dot(w22[m], below[:BLK])
        w32 = -dot(w33[m], dot(l32[m], w22[m]))
        w31 = -dot(w33[m], below[BLK:] + dot(l32[m], w21))
        bands = ((w11[m], w33[m]), (w21, w22[m]), (w31, w32))
        bands = [jnp.concatenate(band, axis=1) for band in bands]
        top = functools.reduce(jnp.maximum, [jnp.max(jnp.abs(band), axis=0, keepdims=True) for band in bands])
        top = jnp.maximum(top, TINY)
        step_ref[m] = top / LEVELS
        for n, band in enumerate(bands):
            out_ref[m, n * BLK : (n + 1) * BLK] = encode(band, LEVELS / top)


def whiten(packed, damp, total):
    count = packed.shape[0]
    return pl.pallas_call(
        functools.partial(whiten_kernel, total, count),
        in_specs=[pl.BlockSpec(memory_space=pltpu.SMEM), pl.BlockSpec(memory_space=pltpu.VMEM)],
        out_specs=[pl.BlockSpec(memory_space=pltpu.VMEM)] * 2,
        out_shape=[
            jax.ShapeDtypeStruct(packed.shape, jnp.int16),
            jax.ShapeDtypeStruct((count, 1, packed.shape[2]), jnp.float32),
        ],
    )(damp, packed)


def flip(index, step):
    return index + step * (1 - 2 * ((index // step) % 2))


def remote(src, dst, sems, slot, device):
    return pltpu.make_async_remote_copy(
        src_ref=src,
        dst_ref=dst,
        send_sem=sems.at[0, slot],
        recv_sem=sems.at[1, slot],
        device_id=device,
        device_id_type=pl.DeviceIdType.MESH,
    )


def greet(heads, dps):
    barrier = pltpu.get_barrier_semaphore()
    for peer in heads:
        pl.semaphore_signal(barrier, inc=1, device_id={"head": peer}, device_id_type=pl.DeviceIdType.MESH)
    for peer in dps:
        pl.semaphore_signal(barrier, inc=1, device_id={"dp": peer}, device_id_type=pl.DeviceIdType.MESH)
    pl.semaphore_wait(barrier, len(heads) + len(dps))


def outer_steps(t, u, odd):
    shape = (8, 2 * BLK)
    low = lax.broadcasted_iota(jnp.int32, shape, 1) < BLK
    sub = lax.broadcasted_iota(jnp.int32, shape, 0)
    t, u = jnp.broadcast_to(t, shape), jnp.broadcast_to(u, shape)
    turned_t, turned_u = pltpu.roll(t, BLK, 1), pltpu.roll(u, BLK, 1)
    down = jnp.where(low, t, turned_u) if odd else jnp.where(low, turned_u, t)
    across = jnp.where(low, u, t) if odd else jnp.where(low, t, u)
    wide = jnp.where(sub == 0, down, 0.0)
    corner = jnp.where(sub == 1, t, jnp.where(sub == 2, turned_t, 0.0))
    left = jnp.concatenate((wide, corner[:, :BLK]), axis=1).astype(jnp.bfloat16)
    third = jnp.where((sub == 2) & ~low, t, 0.0)
    right = jnp.where(sub == 0, across, jnp.where((sub == 1) & low, t, third)).astype(jnp.bfloat16)
    grid = lax.dot_general(left, right, (((0,), (0,)), ((), ())), preferred_element_type=jnp.float32)
    if odd:
        return grid
    return jnp.concatenate((grid[2 * BLK :], grid[: 2 * BLK]), axis=0)


def column_steps(value, odd):
    two = 2 * BLK
    lane = lax.broadcasted_iota(jnp.int32, (BLK, two), 1)
    hit = lane % BLK == lax.broadcasted_iota(jnp.int32, (BLK, two), 0)
    corner, middle = (value[two:], value[BLK:two]) if odd else (value[:BLK], value[BLK:two])
    near = lane < BLK if odd else lane >= BLK
    t = jnp.sum(jnp.where(hit, corner, 0.0), axis=0, keepdims=True)
    u = jnp.sum(jnp.where(hit & near, middle, 0.0), axis=0, keepdims=True)
    scale = (1.0 + 2.0**-8) / math.sqrt(LEVELS - 1.0)
    t, u = (jnp.sqrt(jnp.maximum(d, TINY)) * scale for d in (t, u))
    return tuple(s.astype(jnp.bfloat16).astype(jnp.float32) for s in (t, u))


def put_code(value, odd, code, step, slot, m):
    t, u = column_steps(value, odd)
    step[slot, m, 0:1] = t
    step[slot, m, 1:2] = u
    code[slot, m] = jnp.round(value / outer_steps(t, u, odd)).astype(jnp.int32).astype(jnp.int16)


def get_code(odd, code, step, slot, m):
    return decode(code[slot, m]) * outer_steps(step[slot, m, 0:1], step[slot, m, 1:2], odd)


def get_code_either(odd, code, step, slot, m):
    if isinstance(odd, int):
        return get_code(odd, code, step, slot, m)
    return jnp.where(odd == 1, get_code(1, code, step, slot, m), get_code(0, code, step, slot, m))


def first_step(e, order):
    return next((s for s, j in enumerate(order) if (e >> j) & 1), len(order))


def scatter_kernel(n_head, n_dp, share, waves, rows_ref, weights_ref, out_ref, acc, half, sent, wide, columns, code_out, code_in, step_out, step_in, far_out, far_in, far_step_out, far_step_in, sem_in, sem_0, sem_code, sem_step, sem_far, sem_far_step):
    head = lax.axis_index("head")
    dp = lax.axis_index("dp")
    chunks = n_head // 2
    bits = chunks.bit_length() - 1
    mine = head // 2
    core = head % 2
    per_head = share * n_dp
    mats = per_head // waves
    span = mats * HD
    owners = n_dp // waves
    place = lax.rem(dp, owners)
    peers = [lax.rem(dp + o, n_dp) for o in range(1, n_dp)]
    orders = list(range(bits)), list(range(bits))[::-1]

    def chunk_of(e):
        chunk = mine
        for j in range(bits):
            if (e >> j) & 1:
                chunk = chunk + (1 - 2 * ((mine // (1 << j)) % 2)) * (1 << j)
        return chunk

    groups = [lax.rem(dp // owners + 1 + w, waves) for w in range(waves)]
    tasks = [(w, e) for w in range(waves) for e in range(chunks)[::-1]]
    visits = []
    for w, e in tasks:
        for side in (1 - core, core):
            visits.append((2 * chunk_of(e) + side) * per_head + groups[w] * mats)

    def fetch(v):
        start = pl.multiple_of(visits[v] * HD, 2 * BLK)
        slot = v % DEPTH
        return pltpu.make_async_copy(rows_ref.at[:, pl.ds(start, span)], columns.at[slot], sem_in.at[slot])

    for v in range(DEPTH - 1):
        fetch(v).start()
    wide[...] = jnp.broadcast_to(weights_ref[...], wide.shape)
    greet([flip(head, 1 << j) for j in range(bits + 1)], peers)

    def multiply(v, out):
        if v + DEPTH - 1 < len(visits):
            fetch(v + DEPTH - 1).start()
        fetch(v).wait()

        def pair(i, carry):
            start = pl.multiple_of(i * 2 * HD, 2 * BLK)
            store_pair(columns[v % DEPTH, :, pl.ds(start, 2 * HD)], wide[...], out, 2 * i)
            return carry

        lax.fori_loop(0, mats // 2, pair, 0, unroll=True)

    def swap(k):
        return remote(sent.at[k], half.at[k], sem_0, k, {"head": flip(head, 1)})

    def near_slot(w, e, odd):
        return (w * (chunks - 1) + e - 1) * 2 + odd

    def pass_on(w, e, odd):
        slot = near_slot(w, e, odd)
        peer = {"head": flip(head, 2 << orders[odd][first_step(e, orders[odd])])}
        return [
            remote(code_out.at[slot], code_in.at[slot], sem_code, slot, peer),
            remote(step_out.at[slot], step_in.at[slot], sem_step, slot, peer),
        ]

    def receipts(e, odd):
        order = orders[odd]
        return [e | (1 << order[s]) for s in range(first_step(e, order))]

    def merge(k, odd):
        w, e = tasks[k]
        got = [near_slot(w, other, odd) for other in receipts(e, odd)]
        for other in receipts(e, odd):
            for copy in pass_on(w, other, odd):
                copy.wait()

        def one(i, carry):
            m = 2 * i + odd
            value = acc[k, m] + half[k, m]
            for slot in got:
                value += get_code(odd, code_in, step_in, slot, i)
            if e:
                put_code(value, odd, code_out, step_out, near_slot(w, e, odd), i)
            else:
                if w == waves - 1:
                    acc[k, m] = value
                if w < waves - 1 or owners > 1:
                    put_code(value, odd, far_out, far_step_out, w, m)
            return carry

        lax.fori_loop(0, mats // 2, one, 0, unroll=True)
        if e:
            for copy in pass_on(w, e, odd):
                copy.start()

    def send_far(w):
        flight = []
        for turn in range(w == waves - 1, owners):
            owner = lax.rem(place + turn, owners)
            slot = w * owners + (owners - turn) % owners
            part = pl.ds(owner * share, share)
            peer = {"dp": groups[w] * owners + owner}
            flight.append((remote(far_out.at[w, part], far_in.at[slot], sem_far, slot, peer), slot))
            flight.append((remote(far_step_out.at[w, part], far_step_in.at[slot], sem_far_step, slot, peer), slot))
        for copy, _ in flight:
            copy.start()
        return flight

    plan = {}
    for k, (w, e) in enumerate(tasks):
        for odd in (0, 1):
            waits = len(receipts(e, odd))
            at = k + 1 if not waits else k + LAG * waits
            plan.setdefault(at, []).append((k, odd))
    swapped = set()
    far = []
    for t in range(max(len(tasks), max(plan) + 1)):
        for k, odd in plan.get(t, ()):
            if k not in swapped:
                swap(k).wait()
                swapped.add(k)
            merge(k, odd)
        for k in sorted({k for k, odd in plan.get(t, ()) if tasks[k][1] == 0}):
            far += send_far(tasks[k][0])
        if t < len(tasks):
            multiply(2 * t, sent.at[t])
            swap(t).start()
            multiply(2 * t + 1, acc.at[t])
    for copy, _ in far:
        copy.wait()
    slots = sorted({slot for _, slot in far})
    last = len(tasks) - 1

    def total(m, carry, odd):
        value = acc[last, place * share + m]
        for slot in slots:
            value += get_code_either(odd, far_in, far_step_in, slot, m)
        out_ref[m] = value
        return carry

    if share % 2:
        lax.fori_loop(0, share, lambda m, c: total(m, c, lax.rem(place * share + m, 2)), 0)
    else:

        def both(i, carry):
            return total(2 * i + 1, total(2 * i, carry, 0), 1)

        lax.fori_loop(0, share // 2, both, 0, unroll=True)


def wave_count(per_head, n_dp):
    waves = n_dp
    while waves > 1 and (per_head % waves or (per_head // waves) % 2 or n_dp % waves):
        waves -= 1
    return waves


def gram_sums(projected, weights, n_head, n_dp):
    tokens, width = projected.shape
    mats, rows, lanes = width // HD, HD, 2 * BLK
    per_head = mats // n_head
    share = per_head // n_dp
    chunks = n_head // 2
    waves = wave_count(per_head, n_dp)
    group = per_head // waves
    tasks = waves * chunks
    near = 2 * waves * (chunks - 1)
    f32, i16 = jnp.float32, jnp.int16
    return pl.pallas_call(
        functools.partial(scatter_kernel, n_head, n_dp, share, waves),
        in_specs=[pl.BlockSpec(memory_space=pl.ANY), pl.BlockSpec(memory_space=pltpu.VMEM)],
        out_specs=pl.BlockSpec(memory_space=pltpu.VMEM),
        out_shape=jax.ShapeDtypeStruct((share, rows, lanes), f32),
        scratch_shapes=[
            pltpu.VMEM((tasks, group, rows, lanes), f32),
            pltpu.VMEM((tasks, group, rows, lanes), f32),
            pltpu.VMEM((tasks, group, rows, lanes), f32),
            pltpu.VMEM((tokens, 2 * HD), projected.dtype),
            pltpu.VMEM((DEPTH, tokens, group * HD), projected.dtype),
            pltpu.VMEM((near, group // 2, rows, lanes), i16),
            pltpu.VMEM((near, group // 2, rows, lanes), i16),
            pltpu.VMEM((near, group // 2, 2, lanes), f32),
            pltpu.VMEM((near, group // 2, 2, lanes), f32),
            pltpu.VMEM((waves, group, rows, lanes), i16),
            pltpu.VMEM((n_dp, share, rows, lanes), i16),
            pltpu.VMEM((waves, group, 2, lanes), f32),
            pltpu.VMEM((n_dp, share, 2, lanes), f32),
            pltpu.SemaphoreType.DMA((DEPTH,)),
            pltpu.SemaphoreType.DMA((2, tasks)),
            pltpu.SemaphoreType.DMA((2, near)),
            pltpu.SemaphoreType.DMA((2, near)),
            pltpu.SemaphoreType.DMA((2, n_dp)),
            pltpu.SemaphoreType.DMA((2, n_dp)),
        ],
        compiler_params=pltpu.CompilerParams(collective_id=0, has_side_effects=True, vmem_limit_bytes=60 << 20),
    )(projected, weights)


def gather_kernel(n_dp, share, code_ref, step_ref, codes, steps, sems, step_sems, own_sems):
    dp = lax.axis_index("dp")
    peers = [lax.rem(dp + o, n_dp) for o in range(1, n_dp)]
    mine = pl.ds(dp * share, share)
    own = [
        pltpu.make_async_copy(code_ref, codes.at[mine], own_sems.at[0]),
        pltpu.make_async_copy(step_ref, steps.at[mine], own_sems.at[1]),
    ]
    for copy in own:
        copy.start()
    greet([], peers)
    flight = []
    for o, peer in enumerate(peers):
        flight.append(remote(code_ref, codes.at[mine], sems, o, {"dp": peer}))
        flight.append(remote(step_ref, steps.at[mine], step_sems, o, {"dp": peer}))
    for copy in flight:
        copy.start()
    for copy in own + flight:
        copy.wait()


def gather(code, step, n_dp):
    share = code.shape[0]
    return pl.pallas_call(
        functools.partial(gather_kernel, n_dp, share),
        in_specs=[pl.BlockSpec(memory_space=pltpu.VMEM)] * 2,
        out_specs=[pl.BlockSpec(memory_space=pltpu.VMEM)] * 2,
        out_shape=[
            jax.ShapeDtypeStruct((n_dp * share, *code.shape[1:]), code.dtype),
            jax.ShapeDtypeStruct((n_dp * share, *step.shape[1:]), step.dtype),
        ],
        scratch_shapes=[
            pltpu.SemaphoreType.DMA((2, n_dp - 1)),
            pltpu.SemaphoreType.DMA((2, n_dp - 1)),
            pltpu.SemaphoreType.DMA((2,)),
        ],
        compiler_params=pltpu.CompilerParams(collective_id=1, has_side_effects=True),
    )(code, step)


def unpack_kernel(code_ref, step_ref, out_ref):
    two = 2 * BLK
    left = lax.broadcasted_iota(jnp.int32, (BLK, two), 1) < BLK
    for m in range(out_ref.shape[0]):
        step = step_ref[m]
        top = decode(code_ref[m, :BLK]) * step
        out_ref[m, :BLK, :two] = jnp.where(left, top, 0.0)
        out_ref[m, BLK:, :two] = decode(code_ref[m, BLK:]) * step
        out_ref[m, :two, two:] = jnp.zeros((two, BLK), jnp.float32)
        out_ref[m, two:, two:] = top[:, BLK:]


def unpack(codes, steps):
    mats, rows, lanes = codes.shape
    group = 2
    return pl.pallas_call(
        unpack_kernel,
        grid=(mats // group,),
        in_specs=[
            pl.BlockSpec((group, rows, lanes), lambda i: (i, 0, 0)),
            pl.BlockSpec((group, 1, lanes), lambda i: (i, 0, 0)),
        ],
        out_specs=pl.BlockSpec((group, HD, HD), lambda i: (i, 0, 0)),
        out_shape=jax.ShapeDtypeStruct((mats, HD, HD), jnp.float32),
    )(codes, steps)


def on_device(projected, weight_exp, damp_exp):
    n_head = lax.axis_size("head")
    n_dp = lax.axis_size("dp")
    mats = projected.shape[1] // HD
    share = mats // (n_head * n_dp)
    total = projected.shape[0] * n_head * n_dp
    weights = jnp.exp2(weight_exp.astype(jnp.float32)).astype(jnp.bfloat16)
    owned = gram_sums(projected, weights[:, None], n_head, n_dp)
    first = (lax.axis_index("head") * n_dp + lax.axis_index("dp")) * share
    damp = jnp.exp2(-lax.dynamic_slice_in_dim(damp_exp, first, share, 0).astype(jnp.float32))
    code, step = whiten(owned, damp, float(total))
    codes, steps = gather(code, step, n_dp)
    return unpack(codes, steps)


def solution(mesh):
    return jax.shard_map(
        on_device,
        mesh=mesh,
        in_specs=(P(("dp", "head"), None), P(("dp", "head")), P()),
        out_specs=P("head", None, None),
        check_vma=False,
    )
```

```python
import functools
import math

import jax
import jax.numpy as jnp
from jax import lax
from jax.experimental import pallas as pl
from jax.experimental.pallas import tpu as pltpu
from jax.sharding import PartitionSpec as P

HD = 192
BLK = HD // 3
LEVELS = 32767.0
TINY = 1e-30
DEPTH = 4
LAG = 2
RANK = 8


def store_pair(rows, wide, out, at):
    weighted = rows * wide
    contract = (((0,), (0,)), ((), ()))
    width = 4 * BLK
    first = lax.dot_general(rows[:, :width], weighted[:, :width], contract, preferred_element_type=jnp.float32)
    second = lax.dot_general(rows[:, -width:], weighted[:, -width:], contract, preferred_element_type=jnp.float32)
    two = 2 * BLK
    lanes = lax.broadcasted_iota(jnp.int32, (BLK, two), 1)
    corner = pltpu.roll(first[two : two + BLK, two:], BLK, 1)
    out[at, :BLK, :] = jnp.where(lanes < BLK, first[:BLK, :two], corner)
    out[at, BLK:, :] = first[BLK:HD, :two]
    out[at + 1, :two, :] = second[BLK : BLK + two, two:]
    corner = pltpu.roll(second[BLK:two, :two], BLK, 1)
    out[at + 1, two:, :] = jnp.where(lanes < BLK, corner, second[HD:, two:])


def split(a):
    high = a.astype(jnp.bfloat16)
    return high, (a - high.astype(jnp.float32)).astype(jnp.bfloat16)


def product(a, b, axis):
    (a_high, a_low), (b_high, b_low) = split(a), split(b)
    one = functools.partial(
        lax.dot_general, dimension_numbers=(((1,), (axis,)), ((), ())), preferred_element_type=jnp.float32
    )
    return one(a_high, b_high) + (one(a_high, b_low) + one(a_low, b_high))


def dot(a, b):
    return product(a, b, 0)


def dot_t(a, b):
    return product(a, b, 1)


def inverse_factors(blocks):
    lane = lax.broadcasted_iota(jnp.int32, (8, BLK), 1)
    sub = lax.broadcasted_iota(jnp.int32, (8, BLK), 0)
    groups = BLK // 8
    held = [[block[8 * g : 8 * g + 8] for g in range(groups)] for block in blocks]
    for start in range(0, BLK, RANK):
        own, base = divmod(start, 8)
        spread = [
            [[jnp.broadcast_to(part[:, start + r : start + r + 1], part.shape) for r in range(RANK)] for part in parts[own:]]
            for parts in held
        ]
        for r in range(RANK):
            spot = base + r
            is_k = lane == start + r
            for parts, columns in zip(held, spread):
                scale = 1.0 / columns[0][r][spot : spot + 1]
                row = jnp.where(is_k[:1], 1.0, parts[own][spot : spot + 1]) * scale
                ahead = [columns[0][q][spot : spot + 1] * scale for q in range(r + 1, RANK)]
                for g in range(own, groups):
                    part, column = parts[g], columns[g - own][r]
                    if g == own:
                        if spot == 7:
                            continue
                        column = jnp.where(sub > spot, column, 0.0)
                        kept = jnp.where(is_k & (sub > spot), 0.0, part)
                    else:
                        kept = jnp.where(is_k, 0.0, part)
                    parts[g] = kept - column * row
                    for q, factor in enumerate(ahead, r + 1):
                        columns[g - own][q] -= column * factor
    out = []
    for parts in held:
        rows = []
        for g in range(groups):
            ids = sub + 8 * g
            pivot = jnp.sum(jnp.where(lane == ids, parts[g], 0.0), axis=1, keepdims=True)
            unit = jnp.where(lane < ids, parts[g], jnp.where(lane == ids, 1.0, 0.0))
            rows.append(unit * (1.0 / jnp.sqrt(pivot)))
        out.append(jnp.concatenate(rows, axis=0))
    return out


def unpack_even(got):
    two = 2 * BLK
    return got[:BLK, :BLK], got[BLK:two, BLK:], got[:BLK, BLK:], got[BLK:, :BLK], got[two:, BLK:]


def unpack_odd(got):
    two = 2 * BLK
    return got[two:, :BLK], got[BLK:two, :BLK], got[two:, BLK:], got[:BLK, :].T, got[BLK:two, BLK:].T


def encode(value, scale):
    return jnp.round(value * scale).astype(jnp.int32).astype(jnp.int16)


def decode(code):
    return code.astype(jnp.int32).astype(jnp.float32)


def flip(index, step):
    return index + step * (1 - 2 * ((index // step) % 2))


def remote(src, dst, sems, slot, device):
    return pltpu.make_async_remote_copy(
        src_ref=src,
        dst_ref=dst,
        send_sem=sems.at[0, slot],
        recv_sem=sems.at[1, slot],
        device_id=device,
        device_id_type=pl.DeviceIdType.MESH,
    )


def signal(device):
    barrier = pltpu.get_barrier_semaphore()
    pl.semaphore_signal(barrier, inc=1, device_id=device, device_id_type=pl.DeviceIdType.MESH)


def greet(heads, dps):
    for peer in heads:
        signal({"head": peer})
    for peer in dps:
        signal({"dp": peer})
    pl.semaphore_wait(pltpu.get_barrier_semaphore(), len(heads) + len(dps))


def whiten_kernel(total, n_dp, count, damp_ref, packed_ref, codes, steps, sems, step_sems):
    two = 2 * BLK
    dp = lax.axis_index("dp")
    peers = [lax.rem(dp + o, n_dp) for o in range(1, n_dp)]
    for peer in peers:
        signal({"dp": peer})
    pairs = (count + 1) // 2
    edges = (0, pairs, pairs + count, 2 * (pairs + count))
    diag = lax.broadcasted_iota(jnp.int32, (BLK, BLK), 0) == lax.broadcasted_iota(jnp.int32, (BLK, BLK), 1)
    first = (lax.axis_index("head") * n_dp + dp) * count
    a11, a22, a33, low, a32 = [], [], [], [], []
    for m in range(count):
        got = packed_ref[m] / total
        even = unpack_even(got)
        odd = unpack_odd(got)
        if count % 2 == 0:
            d1, d2, d3, left, corner = odd if m % 2 else even
        else:
            d1, d2, d3, left, corner = (jnp.where((first + m) % 2 == 0, a, b) for a, b in zip(even, odd))
        trace = jnp.sum(jnp.where(diag, d1 + d2 + d3, 0.0), axis=(0, 1), keepdims=True)
        level = trace / HD + 1e-06
        damping = jnp.exp2(-jnp.full((1, 1), damp_ref[first + m]).astype(jnp.float32))
        shift = jnp.where(diag, damping * level, 0.0)
        a11.append(d1 + shift)
        a22.append(d2 + shift)
        a33.append(d3 + shift)
        low.append(left)
        a32.append(corner)
    each = range(count)

    def put(n, left, right):
        block = jnp.concatenate((left, right), axis=1)
        top = jnp.maximum(jnp.max(jnp.abs(block), axis=0, keepdims=True), TINY)
        steps[dp, n] = top / LEVELS
        codes[dp, n * BLK : (n + 1) * BLK] = encode(block, LEVELS / top)

    def put_pairs(n, values):
        for p in range(pairs):
            put(n + p, values[2 * p], values[min(2 * p + 1, count - 1)])

    flight = []

    def send(stage):
        blocks = pl.ds(edges[stage], edges[stage + 1] - edges[stage])
        rows = pl.ds(edges[stage] * BLK, (edges[stage + 1] - edges[stage]) * BLK)
        for o, peer in enumerate(peers):
            slot = stage * len(peers) + o
            code, step = codes.at[dp, rows], steps.at[dp, blocks]
            flight.append(remote(code, code, sems, slot, {"dp": peer}))
            flight.append(remote(step, step, step_sems, slot, {"dp": peer}))
        for copy in flight[-2 * len(peers) :]:
            copy.start()

    w11 = inverse_factors(a11)
    put_pairs(0, w11)
    pl.semaphore_wait(pltpu.get_barrier_semaphore(), len(peers))
    send(0)
    l1 = [dot_t(low[m], w11[m]) for m in each]
    square = [dot_t(l1[m], l1[m]) for m in each]
    w22 = inverse_factors([a22[m] - square[m][:BLK, :BLK] for m in each])
    below = [dot(l1[m], w11[m]) for m in each]
    w21 = [-dot(w22[m], below[m][:BLK]) for m in each]
    for m in each:
        put(edges[1] + m, w21[m], w22[m])
    send(1)
    l32 = [dot_t(a32[m] - square[m][BLK:, :BLK], w22[m]) for m in each]
    w33 = inverse_factors([a33[m] - square[m][BLK:, BLK:] - dot_t(l32[m], l32[m]) for m in each])
    put_pairs(edges[2] + count, w33)
    for m in each:
        w32 = -dot(w33[m], dot(l32[m], w22[m]))
        w31 = -dot(w33[m], below[m][BLK:] + dot(l32[m], w21[m]))
        put(edges[2] + m, w31, w32)
    send(2)
    for copy in flight:
        copy.wait()


def whiten(packed, damp, n_dp, total):
    count, _, lanes = packed.shape
    blocks = 2 * ((count + 1) // 2 + count)
    return pl.pallas_call(
        functools.partial(whiten_kernel, total, n_dp, count),
        in_specs=[pl.BlockSpec(memory_space=pltpu.SMEM), pl.BlockSpec(memory_space=pltpu.VMEM)],
        out_specs=[pl.BlockSpec(memory_space=pltpu.VMEM)] * 2,
        out_shape=[
            jax.ShapeDtypeStruct((n_dp, blocks * BLK, lanes), jnp.int16),
            jax.ShapeDtypeStruct((n_dp, blocks, 1, lanes), jnp.float32),
        ],
        scratch_shapes=[
            pltpu.SemaphoreType.DMA((2, 3 * (n_dp - 1))),
            pltpu.SemaphoreType.DMA((2, 3 * (n_dp - 1))),
        ],
        compiler_params=pltpu.CompilerParams(collective_id=1, has_side_effects=True),
    )(damp, packed)


def outer_steps(t, u, odd):
    shape = (8, 2 * BLK)
    low = lax.broadcasted_iota(jnp.int32, shape, 1) < BLK
    sub = lax.broadcasted_iota(jnp.int32, shape, 0)
    t, u = jnp.broadcast_to(t, shape), jnp.broadcast_to(u, shape)
    turned_t, turned_u = pltpu.roll(t, BLK, 1), pltpu.roll(u, BLK, 1)
    down = jnp.where(low, t, turned_u) if odd else jnp.where(low, turned_u, t)
    across = jnp.where(low, u, t) if odd else jnp.where(low, t, u)
    wide = jnp.where(sub == 0, down, 0.0)
    corner = jnp.where(sub == 1, t, jnp.where(sub == 2, turned_t, 0.0))
    left = jnp.concatenate((wide, corner[:, :BLK]), axis=1).astype(jnp.bfloat16)
    third = jnp.where((sub == 2) & ~low, t, 0.0)
    right = jnp.where(sub == 0, across, jnp.where((sub == 1) & low, t, third)).astype(jnp.bfloat16)
    grid = lax.dot_general(left, right, (((0,), (0,)), ((), ())), preferred_element_type=jnp.float32)
    if odd:
        return grid
    return jnp.concatenate((grid[2 * BLK :], grid[: 2 * BLK]), axis=0)


def column_steps(value, odd):
    two = 2 * BLK
    lane = lax.broadcasted_iota(jnp.int32, (BLK, two), 1)
    hit = lane % BLK == lax.broadcasted_iota(jnp.int32, (BLK, two), 0)
    corner, middle = (value[two:], value[BLK:two]) if odd else (value[:BLK], value[BLK:two])
    near = lane < BLK if odd else lane >= BLK
    t = jnp.sum(jnp.where(hit, corner, 0.0), axis=0, keepdims=True)
    u = jnp.sum(jnp.where(hit & near, middle, 0.0), axis=0, keepdims=True)
    scale = (1.0 + 2.0**-8) / math.sqrt(LEVELS - 1.0)
    t, u = (jnp.sqrt(jnp.maximum(d, TINY)) * scale for d in (t, u))
    return tuple(s.astype(jnp.bfloat16).astype(jnp.float32) for s in (t, u))


def put_code(value, odd, code, step, slot, m):
    t, u = column_steps(value, odd)
    step[slot, m, 0:1] = t
    step[slot, m, 1:2] = u
    code[slot, m] = jnp.round(value / outer_steps(t, u, odd)).astype(jnp.int32).astype(jnp.int16)


def get_code(odd, code, step, slot, m):
    return decode(code[slot, m]) * outer_steps(step[slot, m, 0:1], step[slot, m, 1:2], odd)


def get_code_either(odd, code, step, slot, m):
    if isinstance(odd, int):
        return get_code(odd, code, step, slot, m)
    return jnp.where(odd == 1, get_code(1, code, step, slot, m), get_code(0, code, step, slot, m))


def first_step(e, order):
    return next((s for s, j in enumerate(order) if (e >> j) & 1), len(order))


def scatter_kernel(n_head, n_dp, share, waves, rows_ref, weights_ref, out_ref, acc, half, sent, wide, columns, code_out, code_in, step_out, step_in, far_out, far_in, far_step_out, far_step_in, sem_in, sem_0, sem_code, sem_step, sem_far, sem_far_step):
    head = lax.axis_index("head")
    dp = lax.axis_index("dp")
    chunks = n_head // 2
    bits = chunks.bit_length() - 1
    mine = head // 2
    core = head % 2
    per_head = share * n_dp
    mats = per_head // waves
    span = mats * HD
    owners = n_dp // waves
    place = lax.rem(dp, owners)
    peers = [lax.rem(dp + o, n_dp) for o in range(1, n_dp)]
    orders = list(range(bits)), list(range(bits))[::-1]

    def chunk_of(e):
        chunk = mine
        for j in range(bits):
            if (e >> j) & 1:
                chunk = chunk + (1 - 2 * ((mine // (1 << j)) % 2)) * (1 << j)
        return chunk

    groups = [lax.rem(dp // owners + 1 + w, waves) for w in range(waves)]
    tasks = [(w, e) for w in range(waves) for e in range(chunks)[::-1]]
    visits = []
    for w, e in tasks:
        for side in (1 - core, core):
            visits.append((2 * chunk_of(e) + side) * per_head + groups[w] * mats)

    def fetch(v):
        start = pl.multiple_of(visits[v] * HD, 2 * BLK)
        slot = v % DEPTH
        return pltpu.make_async_copy(rows_ref.at[:, pl.ds(start, span)], columns.at[slot], sem_in.at[slot])

    for v in range(DEPTH - 1):
        fetch(v).start()
    two = 2 * BLK
    for n in range(weights_ref.shape[0]):
        row = jnp.exp2(weights_ref[n : n + 1].astype(jnp.float32))
        column = jnp.broadcast_to(row, (two, two)).T.astype(wide.dtype)
        for lanes in range(0, 2 * HD, two):
            wide[n * two : (n + 1) * two, lanes : lanes + two] = column
    greet([flip(head, 1 << j) for j in range(bits + 1)], peers)

    def multiply(v, out):
        if v + DEPTH - 1 < len(visits):
            fetch(v + DEPTH - 1).start()
        fetch(v).wait()

        def pair(i, carry):
            start = pl.multiple_of(i * 2 * HD, 2 * BLK)
            store_pair(columns[v % DEPTH, :, pl.ds(start, 2 * HD)], wide[...], out, 2 * i)
            return carry

        lax.fori_loop(0, mats // 2, pair, 0, unroll=True)

    def swap(k):
        return remote(sent.at[k], half.at[k], sem_0, k, {"head": flip(head, 1)})

    def near_slot(w, e, odd):
        return (w * (chunks - 1) + e - 1) * 2 + odd

    def pass_on(w, e, odd):
        slot = near_slot(w, e, odd)
        peer = {"head": flip(head, 2 << orders[odd][first_step(e, orders[odd])])}
        return [
            remote(code_out.at[slot], code_in.at[slot], sem_code, slot, peer),
            remote(step_out.at[slot], step_in.at[slot], sem_step, slot, peer),
        ]

    def receipts(e, odd):
        order = orders[odd]
        return [e | (1 << order[s]) for s in range(first_step(e, order))]

    def merge(k, odd):
        w, e = tasks[k]
        got = [near_slot(w, other, odd) for other in receipts(e, odd)]
        for other in receipts(e, odd):
            for copy in pass_on(w, other, odd):
                copy.wait()

        def one(i, carry):
            m = 2 * i + odd
            value = acc[k, m] + half[k, m]
            for slot in got:
                value += get_code(odd, code_in, step_in, slot, i)
            if e:
                put_code(value, odd, code_out, step_out, near_slot(w, e, odd), i)
            else:
                if w == waves - 1:
                    acc[k, m] = value
                if w < waves - 1 or owners > 1:
                    put_code(value, odd, far_out, far_step_out, w, m)
            return carry

        lax.fori_loop(0, mats // 2, one, 0, unroll=True)
        if e:
            for copy in pass_on(w, e, odd):
                copy.start()

    def send_far(w):
        flight = []
        for turn in range(w == waves - 1, owners):
            owner = lax.rem(place + turn, owners)
            slot = w * owners + (owners - turn) % owners
            part = pl.ds(owner * share, share)
            peer = {"dp": groups[w] * owners + owner}
            flight.append((remote(far_out.at[w, part], far_in.at[slot], sem_far, slot, peer), slot))
            flight.append((remote(far_step_out.at[w, part], far_step_in.at[slot], sem_far_step, slot, peer), slot))
        for copy, _ in flight:
            copy.start()
        return flight

    plan = {}
    for k, (w, e) in enumerate(tasks):
        for odd in (0, 1):
            waits = len(receipts(e, odd))
            at = k + 2 + LAG * waits
            plan.setdefault(at, []).append((k, odd))
    swapped = set()
    far = []
    for t in range(max(len(tasks), max(plan) + 1)):
        for k, odd in plan.get(t, ()):
            if k not in swapped:
                swap(k).wait()
                swapped.add(k)
            merge(k, odd)
        for k in sorted({k for k, odd in plan.get(t, ()) if tasks[k][1] == 0}):
            far += send_far(tasks[k][0])
        if t < len(tasks):
            multiply(2 * t, sent.at[t])
            swap(t).start()
            multiply(2 * t + 1, acc.at[t])
    for copy, _ in far:
        copy.wait()
    slots = sorted({slot for _, slot in far})
    last = len(tasks) - 1

    def total(m, carry, odd):
        value = acc[last, place * share + m]
        for slot in slots:
            value += get_code_either(odd, far_in, far_step_in, slot, m)
        out_ref[m] = value
        return carry

    if share % 2:
        lax.fori_loop(0, share, lambda m, c: total(m, c, lax.rem(place * share + m, 2)), 0)
    else:

        def both(i, carry):
            return total(2 * i + 1, total(2 * i, carry, 0), 1)

        lax.fori_loop(0, share // 2, both, 0, unroll=True)


def wave_count(per_head, n_dp):
    waves = n_dp
    while waves > 1 and (per_head % waves or (per_head // waves) % 2 or n_dp % waves):
        waves -= 1
    return waves


def gram_sums(projected, weights, n_head, n_dp):
    tokens, width = projected.shape
    mats, rows, lanes = width // HD, HD, 2 * BLK
    per_head = mats // n_head
    share = per_head // n_dp
    chunks = n_head // 2
    waves = wave_count(per_head, n_dp)
    group = per_head // waves
    tasks = waves * chunks
    near = 2 * waves * (chunks - 1)
    f32, i16 = jnp.float32, jnp.int16
    return pl.pallas_call(
        functools.partial(scatter_kernel, n_head, n_dp, share, waves),
        in_specs=[pl.BlockSpec(memory_space=pl.ANY), pl.BlockSpec(memory_space=pltpu.VMEM)],
        out_specs=pl.BlockSpec(memory_space=pltpu.VMEM),
        out_shape=jax.ShapeDtypeStruct((share, rows, lanes), f32),
        scratch_shapes=[
            pltpu.VMEM((tasks, group, rows, lanes), f32),
            pltpu.VMEM((tasks, group, rows, lanes), f32),
            pltpu.VMEM((tasks, group, rows, lanes), f32),
            pltpu.VMEM((tokens, 2 * HD), projected.dtype),
            pltpu.VMEM((DEPTH, tokens, group * HD), projected.dtype),
            pltpu.VMEM((near, group // 2, rows, lanes), i16),
            pltpu.VMEM((near, group // 2, rows, lanes), i16),
            pltpu.VMEM((near, group // 2, 2, lanes), f32),
            pltpu.VMEM((near, group // 2, 2, lanes), f32),
            pltpu.VMEM((waves, group, rows, lanes), i16),
            pltpu.VMEM((n_dp, share, rows, lanes), i16),
            pltpu.VMEM((waves, group, 2, lanes), f32),
            pltpu.VMEM((n_dp, share, 2, lanes), f32),
            pltpu.SemaphoreType.DMA((DEPTH,)),
            pltpu.SemaphoreType.DMA((2, tasks)),
            pltpu.SemaphoreType.DMA((2, near)),
            pltpu.SemaphoreType.DMA((2, near)),
            pltpu.SemaphoreType.DMA((2, n_dp)),
            pltpu.SemaphoreType.DMA((2, n_dp)),
        ],
        compiler_params=pltpu.CompilerParams(collective_id=0, has_side_effects=True, vmem_limit_bytes=60 << 20),
    )(projected, weights)


def unpack_kernel(count, code_ref, step_ref, out_ref):
    two = 2 * BLK
    pairs = (count + 1) // 2
    left = lax.broadcasted_iota(jnp.int32, (BLK, two), 1) < BLK
    for d in range(code_ref.shape[0]):

        def block(n, d=d):
            return decode(code_ref[d, n * BLK : (n + 1) * BLK]) * step_ref[d, n]

        for m in range(count):
            at = d * count + m
            top, last = block(m // 2), block(2 * pairs + 2 * count - pairs + m // 2)
            if m % 2:
                top, last = pltpu.roll(top, BLK, 1), pltpu.roll(last, BLK, 1)
            out_ref[at, :BLK, :two] = jnp.where(left, top, 0.0)
            out_ref[at, BLK:two, :two] = block(pairs + m)
            out_ref[at, two:, :two] = block(pairs + count + m)
            out_ref[at, :two, two:] = jnp.zeros((two, BLK), jnp.float32)
            out_ref[at, two:, two:] = last[:, :BLK]


def unpack(codes, steps, count):
    n_dp, rows, lanes = codes.shape
    group = n_dp // 2 if n_dp % 2 == 0 else n_dp
    return pl.pallas_call(
        functools.partial(unpack_kernel, count),
        grid=(n_dp // group,),
        in_specs=[
            pl.BlockSpec((group, rows, lanes), lambda i: (i, 0, 0)),
            pl.BlockSpec((group, rows // BLK, 1, lanes), lambda i: (i, 0, 0, 0)),
        ],
        out_specs=pl.BlockSpec((group * count, HD, HD), lambda i: (i, 0, 0)),
        out_shape=jax.ShapeDtypeStruct((n_dp * count, HD, HD), jnp.float32),
    )(codes, steps)


def on_device(projected, weight_exp, damp_exp):
    n_head = lax.axis_size("head")
    n_dp = lax.axis_size("dp")
    total = projected.shape[0] * n_head * n_dp
    owned = gram_sums(projected, weight_exp.reshape(-1, 2 * BLK), n_head, n_dp)
    codes, steps = whiten(owned, damp_exp, n_dp, float(total))
    return unpack(codes, steps, owned.shape[0])


def solution(mesh):
    return jax.shard_map(
        on_device,
        mesh=mesh,
        in_specs=(P(("dp", "head"), None), P(("dp", "head")), P()),
        out_specs=P("head", None, None),
        check_vma=False,
    )
```

```python
import functools
import math

import jax
import jax.numpy as jnp
from jax import lax
from jax.experimental import pallas as pl
from jax.experimental.pallas import tpu as pltpu
from jax.sharding import PartitionSpec as P

HD = 192
BLK = HD // 3
LEVELS = 32767.0
TINY = 1e-30
DEPTH = 4
LAG = 2
RANK = 8
HALF = BLK // 2


def store_pair(rows, wide, out, at):
    weighted = rows * wide
    contract = (((0,), (0,)), ((), ()))
    width = 4 * BLK
    first = lax.dot_general(rows[:, :width], weighted[:, :width], contract, preferred_element_type=jnp.float32)
    second = lax.dot_general(rows[:, -width:], weighted[:, -width:], contract, preferred_element_type=jnp.float32)
    two = 2 * BLK
    lanes = lax.broadcasted_iota(jnp.int32, (BLK, two), 1)
    corner = pltpu.roll(first[two : two + BLK, two:], BLK, 1)
    out[at, :BLK, :] = jnp.where(lanes < BLK, first[:BLK, :two], corner)
    out[at, BLK:, :] = first[BLK:HD, :two]
    out[at + 1, :two, :] = second[BLK : BLK + two, two:]
    corner = pltpu.roll(second[BLK:two, :two], BLK, 1)
    out[at + 1, two:, :] = jnp.where(lanes < BLK, corner, second[HD:, two:])


def split(a):
    high = a.astype(jnp.bfloat16)
    return high, (a - high.astype(jnp.float32)).astype(jnp.bfloat16)


def product(a, b, axis):
    (a_high, a_low), (b_high, b_low) = split(a), split(b)
    one = functools.partial(
        lax.dot_general, dimension_numbers=(((1,), (axis,)), ((), ())), preferred_element_type=jnp.float32
    )
    return one(a_high, b_high) + (one(a_high, b_low) + one(a_low, b_high))


def dot(a, b):
    return product(a, b, 0)


def dot_t(a, b):
    return product(a, b, 1)


def inverse_halves(blocks):
    lane = lax.broadcasted_iota(jnp.int32, (8, BLK), 1)
    sub = lax.broadcasted_iota(jnp.int32, (8, BLK), 0)
    groups = BLK // 8
    held = [[block[8 * g : 8 * g + 8] for g in range(groups)] for block in blocks]
    for start in range(0, BLK, RANK):
        if start == HALF:
            yield finished(held, 0, groups // 2)
        own, base = divmod(start, 8)
        spread = [
            [[jnp.broadcast_to(part[:, start + r : start + r + 1], part.shape) for r in range(RANK)] for part in parts[own:]]
            for parts in held
        ]
        for r in range(RANK):
            spot = base + r
            is_k = lane == start + r
            for parts, columns in zip(held, spread):
                scale = 1.0 / columns[0][r][spot : spot + 1]
                row = jnp.where(is_k[:1], 1.0, parts[own][spot : spot + 1]) * scale
                ahead = [columns[0][q][spot : spot + 1] * scale for q in range(r + 1, RANK)]
                for g in range(own, groups):
                    part, column = parts[g], columns[g - own][r]
                    if g == own:
                        if spot == 7:
                            continue
                        column = jnp.where(sub > spot, column, 0.0)
                        kept = jnp.where(is_k & (sub > spot), 0.0, part)
                    else:
                        kept = jnp.where(is_k, 0.0, part)
                    parts[g] = kept - column * row
                    for q, factor in enumerate(ahead, r + 1):
                        columns[g - own][q] -= column * factor
    yield finished(held, groups // 2, groups)


def finished(held, begin, end):
    lane = lax.broadcasted_iota(jnp.int32, (8, BLK), 1)
    sub = lax.broadcasted_iota(jnp.int32, (8, BLK), 0)
    out = []
    for parts in held:
        rows = []
        for g in range(begin, end):
            ids = sub + 8 * g
            pivot = jnp.sum(jnp.where(lane == ids, parts[g], 0.0), axis=1, keepdims=True)
            unit = jnp.where(lane < ids, parts[g], jnp.where(lane == ids, 1.0, 0.0))
            rows.append(unit * (1.0 / jnp.sqrt(pivot)))
        out.append(jnp.concatenate(rows, axis=0))
    return out


def stage_starts(count):
    pairs = (count + 1) // 2
    starts = [0]
    for cells in (pairs, pairs, count, count, count + pairs, count + pairs):
        starts.append(starts[-1] + cells)
    return starts


def joined(halves):
    return [jnp.concatenate(both, axis=0) for both in zip(*halves)]


def unpack_even(got):
    two = 2 * BLK
    return got[:BLK, :BLK], got[BLK:two, BLK:], got[:BLK, BLK:], got[BLK:, :BLK], got[two:, BLK:]


def unpack_odd(got):
    two = 2 * BLK
    return got[two:, :BLK], got[BLK:two, :BLK], got[two:, BLK:], got[:BLK, :].T, got[BLK:two, BLK:].T


def encode(value, scale):
    return jnp.round(value * scale).astype(jnp.int32).astype(jnp.int16)


def decode(code):
    return code.astype(jnp.int32).astype(jnp.float32)


def flip(index, step):
    return index + step * (1 - 2 * ((index // step) % 2))


def remote(src, dst, sems, slot, device):
    return pltpu.make_async_remote_copy(
        src_ref=src,
        dst_ref=dst,
        send_sem=sems.at[0, slot],
        recv_sem=sems.at[1, slot],
        device_id=device,
        device_id_type=pl.DeviceIdType.MESH,
    )


def signal(device):
    barrier = pltpu.get_barrier_semaphore()
    pl.semaphore_signal(barrier, inc=1, device_id=device, device_id_type=pl.DeviceIdType.MESH)


def greet(heads, dps):
    for peer in heads:
        signal({"head": peer})
    for peer in dps:
        signal({"dp": peer})
    pl.semaphore_wait(pltpu.get_barrier_semaphore(), len(heads) + len(dps))


def whiten_owned(total, n_dp, count, damp_ref, packed_ref, codes, steps, sems, step_sems):
    dp = lax.axis_index("dp")
    peers = [lax.rem(dp + o, n_dp) for o in range(1, n_dp)]
    pairs = (count + 1) // 2
    starts = stage_starts(count)
    diag = lax.broadcasted_iota(jnp.int32, (BLK, BLK), 0) == lax.broadcasted_iota(jnp.int32, (BLK, BLK), 1)
    first = (lax.axis_index("head") * n_dp + dp) * count
    a11, a22, a33, low, a32 = [], [], [], [], []
    for m in range(count):
        got = packed_ref[m] / total
        even = unpack_even(got)
        odd = unpack_odd(got)
        if count % 2 == 0:
            d1, d2, d3, left, corner = odd if m % 2 else even
        else:
            d1, d2, d3, left, corner = (jnp.where((first + m) % 2 == 0, a, b) for a, b in zip(even, odd))
        trace = jnp.sum(jnp.where(diag, d1 + d2 + d3, 0.0), axis=(0, 1), keepdims=True)
        level = trace / HD + 1e-06
        damping = jnp.exp2(-jnp.full((1, 1), damp_ref[first + m]).astype(jnp.float32))
        shift = jnp.where(diag, damping * level, 0.0)
        a11.append(d1 + shift)
        a22.append(d2 + shift)
        a33.append(d3 + shift)
        low.append(left)
        a32.append(corner)
    each = range(count)

    def put(n, left, right):
        block = jnp.concatenate((left, right), axis=1)
        top = jnp.maximum(jnp.max(jnp.abs(block), axis=0, keepdims=True), TINY)
        steps[dp, n] = top / LEVELS
        codes[dp, n * HALF : (n + 1) * HALF] = encode(block, LEVELS / top)

    def put_pairs(n, values):
        for p in range(pairs):
            put(n + p, values[2 * p], values[min(2 * p + 1, count - 1)])

    flight = []

    def send(stage):
        cells = starts[stage + 1] - starts[stage]
        blocks = pl.ds(starts[stage], cells)
        rows = pl.ds(starts[stage] * HALF, cells * HALF)
        for o, peer in enumerate(peers):
            slot = stage * len(peers) + o
            code, step = codes.at[dp, rows], steps.at[dp, blocks]
            flight.append(remote(code, code, sems, slot, {"dp": peer}))
            flight.append(remote(step, step, step_sems, slot, {"dp": peer}))
        for copy in flight[-2 * len(peers) :]:
            copy.start()

    halves = []
    for h, half in enumerate(inverse_halves(a11)):
        put_pairs(starts[h], half)
        send(h)
        halves.append(half)
    w11 = joined(halves)
    l1 = [dot_t(low[m], w11[m]) for m in each]
    square = [dot_t(l1[m], l1[m]) for m in each]
    below = [dot(l1[m], w11[m]) for m in each]
    halves, lefts = [], []
    for h, half in enumerate(inverse_halves([a22[m] - square[m][:BLK, :BLK] for m in each])):
        left = [-dot(half[m], below[m][:BLK]) for m in each]
        for m in each:
            put(starts[2 + h] + m, left[m], half[m])
        send(2 + h)
        halves.append(half)
        lefts.append(left)
    w22, w21 = joined(halves), joined(lefts)
    l32 = [dot_t(a32[m] - square[m][BLK:, :BLK], w22[m]) for m in each]
    right = [dot(l32[m], w22[m]) for m in each]
    left = [below[m][BLK:] + dot(l32[m], w21[m]) for m in each]
    rest = [a33[m] - square[m][BLK:, BLK:] - dot_t(l32[m], l32[m]) for m in each]
    for h, half in enumerate(inverse_halves(rest)):
        for m in each:
            put(starts[4 + h] + m, -dot(half[m], left[m]), -dot(half[m], right[m]))
        put_pairs(starts[4 + h] + count, half)
        send(4 + h)
    for copy in flight:
        copy.wait()


def outer_steps(t, u, odd):
    shape = (8, 2 * BLK)
    low = lax.broadcasted_iota(jnp.int32, shape, 1) < BLK
    sub = lax.broadcasted_iota(jnp.int32, shape, 0)
    t, u = jnp.broadcast_to(t, shape), jnp.broadcast_to(u, shape)
    turned_t, turned_u = pltpu.roll(t, BLK, 1), pltpu.roll(u, BLK, 1)
    down = jnp.where(low, t, turned_u) if odd else jnp.where(low, turned_u, t)
    across = jnp.where(low, u, t) if odd else jnp.where(low, t, u)
    wide = jnp.where(sub == 0, down, 0.0)
    corner = jnp.where(sub == 1, t, jnp.where(sub == 2, turned_t, 0.0))
    left = jnp.concatenate((wide, corner[:, :BLK]), axis=1).astype(jnp.bfloat16)
    third = jnp.where((sub == 2) & ~low, t, 0.0)
    right = jnp.where(sub == 0, across, jnp.where((sub == 1) & low, t, third)).astype(jnp.bfloat16)
    grid = lax.dot_general(left, right, (((0,), (0,)), ((), ())), preferred_element_type=jnp.float32)
    if odd:
        return grid
    return jnp.concatenate((grid[2 * BLK :], grid[: 2 * BLK]), axis=0)


def column_steps(value, odd):
    two = 2 * BLK
    lane = lax.broadcasted_iota(jnp.int32, (BLK, two), 1)
    hit = lane % BLK == lax.broadcasted_iota(jnp.int32, (BLK, two), 0)
    corner, middle = (value[two:], value[BLK:two]) if odd else (value[:BLK], value[BLK:two])
    near = lane < BLK if odd else lane >= BLK
    t = jnp.sum(jnp.where(hit, corner, 0.0), axis=0, keepdims=True)
    u = jnp.sum(jnp.where(hit & near, middle, 0.0), axis=0, keepdims=True)
    scale = (1.0 + 2.0**-8) / math.sqrt(LEVELS - 1.0)
    t, u = (jnp.sqrt(jnp.maximum(d, TINY)) * scale for d in (t, u))
    return tuple(s.astype(jnp.bfloat16).astype(jnp.float32) for s in (t, u))


def put_code(value, odd, code, step, slot, m):
    t, u = column_steps(value, odd)
    step[slot, m, 0:1] = t
    step[slot, m, 1:2] = u
    code[slot, m] = jnp.round(value / outer_steps(t, u, odd)).astype(jnp.int32).astype(jnp.int16)


def get_code(odd, code, step, slot, m):
    return decode(code[slot, m]) * outer_steps(step[slot, m, 0:1], step[slot, m, 1:2], odd)


def get_code_either(odd, code, step, slot, m):
    if isinstance(odd, int):
        return get_code(odd, code, step, slot, m)
    return jnp.where(odd == 1, get_code(1, code, step, slot, m), get_code(0, code, step, slot, m))


def first_step(e, order):
    return next((s for s, j in enumerate(order) if (e >> j) & 1), len(order))


def scatter_kernel(n_head, n_dp, share, waves, total_tokens, rows_ref, weights_ref, damp_ref, codes, steps, owned, acc, half, sent, wide, columns, code_out, code_in, step_out, step_in, far_out, far_in, far_step_out, far_step_in, sem_in, sem_0, sem_code, sem_step, sem_far, sem_far_step, sem_out, sem_out_step):
    head = lax.axis_index("head")
    dp = lax.axis_index("dp")
    chunks = n_head // 2
    bits = chunks.bit_length() - 1
    mine = head // 2
    core = head % 2
    per_head = share * n_dp
    mats = per_head // waves
    span = mats * HD
    owners = n_dp // waves
    place = lax.rem(dp, owners)
    peers = [lax.rem(dp + o, n_dp) for o in range(1, n_dp)]
    orders = list(range(bits)), list(range(bits))[::-1]

    def chunk_of(e):
        chunk = mine
        for j in range(bits):
            if (e >> j) & 1:
                chunk = chunk + (1 - 2 * ((mine // (1 << j)) % 2)) * (1 << j)
        return chunk

    groups = [lax.rem(dp // owners + 1 + w, waves) for w in range(waves)]
    tasks = [(w, e) for w in range(waves) for e in range(chunks)[::-1]]
    visits = []
    for w, e in tasks:
        for side in (1 - core, core):
            visits.append((2 * chunk_of(e) + side) * per_head + groups[w] * mats)

    def fetch(v):
        start = pl.multiple_of(visits[v] * HD, 2 * BLK)
        slot = v % DEPTH
        return pltpu.make_async_copy(rows_ref.at[:, pl.ds(start, span)], columns.at[slot], sem_in.at[slot])

    for v in range(DEPTH - 1):
        fetch(v).start()
    two = 2 * BLK
    for n in range(weights_ref.shape[0]):
        row = jnp.exp2(weights_ref[n : n + 1].astype(jnp.float32))
        column = jnp.broadcast_to(row, (two, two)).T.astype(wide.dtype)
        for lanes in range(0, 2 * HD, two):
            wide[n * two : (n + 1) * two, lanes : lanes + two] = column
    greet([flip(head, 1 << j) for j in range(bits + 1)], peers)

    def multiply(v, out):
        if v + DEPTH - 1 < len(visits):
            fetch(v + DEPTH - 1).start()
        fetch(v).wait()

        def pair(i, carry):
            start = pl.multiple_of(i * 2 * HD, 2 * BLK)
            store_pair(columns[v % DEPTH, :, pl.ds(start, 2 * HD)], wide[...], out, 2 * i)
            return carry

        lax.fori_loop(0, mats // 2, pair, 0, unroll=True)

    def swap(k):
        return remote(sent.at[k], half.at[k], sem_0, k, {"head": flip(head, 1)})

    def near_slot(w, e, odd):
        return (w * (chunks - 1) + e - 1) * 2 + odd

    def pass_on(w, e, odd):
        slot = near_slot(w, e, odd)
        peer = {"head": flip(head, 2 << orders[odd][first_step(e, orders[odd])])}
        return [
            remote(code_out.at[slot], code_in.at[slot], sem_code, slot, peer),
            remote(step_out.at[slot], step_in.at[slot], sem_step, slot, peer),
        ]

    def receipts(e, odd):
        order = orders[odd]
        return [e | (1 << order[s]) for s in range(first_step(e, order))]

    def merge(k, odd):
        w, e = tasks[k]
        got = [near_slot(w, other, odd) for other in receipts(e, odd)]
        for other in receipts(e, odd):
            for copy in pass_on(w, other, odd):
                copy.wait()

        def one(i, carry):
            m = 2 * i + odd
            value = acc[k, m] + half[k, m]
            for slot in got:
                value += get_code(odd, code_in, step_in, slot, i)
            if e:
                put_code(value, odd, code_out, step_out, near_slot(w, e, odd), i)
            else:
                if w == waves - 1:
                    acc[k, m] = value
                if w < waves - 1 or owners > 1:
                    put_code(value, odd, far_out, far_step_out, w, m)
            return carry

        lax.fori_loop(0, mats // 2, one, 0, unroll=True)
        if e:
            for copy in pass_on(w, e, odd):
                copy.start()

    def send_far(w):
        flight = []
        for turn in range(w == waves - 1, owners):
            owner = lax.rem(place + turn, owners)
            slot = w * owners + (owners - turn) % owners
            part = pl.ds(owner * share, share)
            peer = {"dp": groups[w] * owners + owner}
            flight.append((remote(far_out.at[w, part], far_in.at[slot], sem_far, slot, peer), slot))
            flight.append((remote(far_step_out.at[w, part], far_step_in.at[slot], sem_far_step, slot, peer), slot))
        for copy, _ in flight:
            copy.start()
        return flight

    plan = {}
    for k, (w, e) in enumerate(tasks):
        for odd in (0, 1):
            waits = len(receipts(e, odd))
            at = k + 2 + LAG * waits
            plan.setdefault(at, []).append((k, odd))
    swapped = set()
    far = []
    for t in range(max(len(tasks), max(plan) + 1)):
        for k, odd in plan.get(t, ()):
            if k not in swapped:
                swap(k).wait()
                swapped.add(k)
            merge(k, odd)
        for k in sorted({k for k, odd in plan.get(t, ()) if tasks[k][1] == 0}):
            far += send_far(tasks[k][0])
        if t < len(tasks):
            multiply(2 * t, sent.at[t])
            swap(t).start()
            multiply(2 * t + 1, acc.at[t])
    for copy, _ in far:
        copy.wait()
    slots = sorted({slot for _, slot in far})
    last = len(tasks) - 1

    def total(m, carry, odd):
        value = acc[last, place * share + m]
        for slot in slots:
            value += get_code_either(odd, far_in, far_step_in, slot, m)
        owned[m] = value
        return carry

    if share % 2:
        lax.fori_loop(0, share, lambda m, c: total(m, c, lax.rem(place * share + m, 2)), 0)
    else:

        def both(i, carry):
            return total(2 * i + 1, total(2 * i, carry, 0), 1)

        lax.fori_loop(0, share // 2, both, 0, unroll=True)
    whiten_owned(total_tokens, n_dp, share, damp_ref, owned, codes, steps, sem_out, sem_out_step)


def wave_count(per_head, n_dp):
    waves = n_dp
    while waves > 1 and (per_head % waves or (per_head // waves) % 2 or n_dp % waves):
        waves -= 1
    return waves


def whitened_codes(projected, weights, damp, n_head, n_dp):
    tokens, width = projected.shape
    mats, rows, lanes = width // HD, HD, 2 * BLK
    per_head = mats // n_head
    share = per_head // n_dp
    chunks = n_head // 2
    waves = wave_count(per_head, n_dp)
    group = per_head // waves
    tasks = waves * chunks
    near = 2 * waves * (chunks - 1)
    cells = stage_starts(share)[-1]
    f32, i16 = jnp.float32, jnp.int16
    return pl.pallas_call(
        functools.partial(scatter_kernel, n_head, n_dp, share, waves, float(tokens * n_head * n_dp)),
        in_specs=[pl.BlockSpec(memory_space=space) for space in (pl.ANY, pltpu.VMEM, pltpu.SMEM)],
        out_specs=[pl.BlockSpec(memory_space=pltpu.VMEM)] * 2,
        out_shape=[
            jax.ShapeDtypeStruct((n_dp, cells * HALF, lanes), i16),
            jax.ShapeDtypeStruct((n_dp, cells, 1, lanes), f32),
        ],
        scratch_shapes=[
            pltpu.VMEM((share, rows, lanes), f32),
            pltpu.VMEM((tasks, group, rows, lanes), f32),
            pltpu.VMEM((tasks, group, rows, lanes), f32),
            pltpu.VMEM((tasks, group, rows, lanes), f32),
            pltpu.VMEM((tokens, 2 * HD), projected.dtype),
            pltpu.VMEM((DEPTH, tokens, group * HD), projected.dtype),
            pltpu.VMEM((near, group // 2, rows, lanes), i16),
            pltpu.VMEM((near, group // 2, rows, lanes), i16),
            pltpu.VMEM((near, group // 2, 2, lanes), f32),
            pltpu.VMEM((near, group // 2, 2, lanes), f32),
            pltpu.VMEM((waves, group, rows, lanes), i16),
            pltpu.VMEM((n_dp, share, rows, lanes), i16),
            pltpu.VMEM((waves, group, 2, lanes), f32),
            pltpu.VMEM((n_dp, share, 2, lanes), f32),
            pltpu.SemaphoreType.DMA((DEPTH,)),
            pltpu.SemaphoreType.DMA((2, tasks)),
            pltpu.SemaphoreType.DMA((2, near)),
            pltpu.SemaphoreType.DMA((2, near)),
            pltpu.SemaphoreType.DMA((2, n_dp)),
            pltpu.SemaphoreType.DMA((2, n_dp)),
            pltpu.SemaphoreType.DMA((2, 6 * (n_dp - 1))),
            pltpu.SemaphoreType.DMA((2, 6 * (n_dp - 1))),
        ],
        compiler_params=pltpu.CompilerParams(collective_id=0, has_side_effects=True, vmem_limit_bytes=60 << 20),
    )(projected, weights, damp)


def unpack_kernel(count, code_ref, step_ref, out_ref):
    two = 2 * BLK
    starts = stage_starts(count)
    left = lax.broadcasted_iota(jnp.int32, (BLK, two), 1) < BLK
    for d in range(code_ref.shape[0]):

        def block(stage, n, d=d):
            cells = [starts[stage + h] + n for h in range(2)]
            parts = [decode(code_ref[d, c * HALF : (c + 1) * HALF]) * step_ref[d, c] for c in cells]
            return jnp.concatenate(parts, axis=0)

        for m in range(count):
            at = d * count + m
            top, last = block(0, m // 2), block(4, count + m // 2)
            if m % 2:
                top, last = pltpu.roll(top, BLK, 1), pltpu.roll(last, BLK, 1)
            out_ref[at, :BLK, :two] = jnp.where(left, top, 0.0)
            out_ref[at, BLK:two, :two] = block(2, m)
            out_ref[at, two:, :two] = block(4, m)
            out_ref[at, :two, two:] = jnp.zeros((two, BLK), jnp.float32)
            out_ref[at, two:, two:] = last[:, :BLK]


def unpack(codes, steps, count):
    n_dp, rows, lanes = codes.shape
    group = n_dp // 2 if n_dp % 2 == 0 else n_dp
    return pl.pallas_call(
        functools.partial(unpack_kernel, count),
        grid=(n_dp // group,),
        in_specs=[
            pl.BlockSpec((group, rows, lanes), lambda i: (i, 0, 0)),
            pl.BlockSpec((group, rows // HALF, 1, lanes), lambda i: (i, 0, 0, 0)),
        ],
        out_specs=pl.BlockSpec((group * count, HD, HD), lambda i: (i, 0, 0)),
        out_shape=jax.ShapeDtypeStruct((n_dp * count, HD, HD), jnp.float32),
    )(codes, steps)


def on_device(projected, weight_exp, damp_exp):
    n_head = lax.axis_size("head")
    n_dp = lax.axis_size("dp")
    share = projected.shape[1] // HD // (n_head * n_dp)
    codes, steps = whitened_codes(projected, weight_exp.reshape(-1, 2 * BLK), damp_exp, n_head, n_dp)
    return unpack(codes, steps, share)


def solution(mesh):
    return jax.shard_map(
        on_device,
        mesh=mesh,
        in_specs=(P(("dp", "head"), None), P(("dp", "head")), P()),
        out_specs=P("head", None, None),
        check_vma=False,
    )
```
